32 devices in a mesh: lat: 4 (over y, x), lon: 8 (over z, core).
Axes of the slice: x: 2, y: 2, z: 4, core: 2. Of those that a mesh axis runs over, the one named last changes fastest.
Arguments:
- right_side: float32 [512, 1024], P('lat', 'lon'), may hold values from -8 to 8
- surface_term: float32 [512, 1024], P('lat', 'lon'), may hold values from 0.0002 to 0.002
- east_coupling: float32 [512, 1024], P('lat', 'lon'), may hold values from 0.3 to 3
- north_coupling: float32 [512, 1024], P('lat', 'lon'), may hold values from 0.3 to 3
- neast_coupling: float32 [512, 1024], P('lat', 'lon'), may hold values from 0.1 to 0.5
- nwest_coupling: float32 [512, 1024], P('lat', 'lon'), may hold values from 0.1 to 0.5
- land_sea: int32 [512, 1024], P('lat', 'lon'), may hold values from 0 to 1, as said below
- fold_map: int32 [1024], P('lon'), may hold values from 0 to 1023, as said below
Outputs:
- solution: float32 [512, 1024], P('lat', 'lon')
- residual: float32 [512, 1024], P('lat', 'lon')
The draws below stay inside these ranges and needn't reach their ends.
Inputs may be any that keep to these rules, and one draw needn't show every extreme that they name: fold_map[j] = (c - j) mod 1024 for one odd c: an involution of the columns with no fixed point. land_sea is 0 or 1; land lies in bands of 8 columns, each over one range of rows.
All inputs are finite; a program needn't handle non-finite values.
Results may differ from the reference program's by a relative error of at most 0.0015.
Values sent between devices are 32-bit elements.
A program may use at most 64 MiB of HBM per device.

```python
import math
import jax
import jax.numpy as jnp
from jax import lax

ITERS = 8
NLAT = 512
NLON = 1024


def draw_right_side(key, part):
    noise_key, scale_key = jax.random.split(jax.random.fold_in(key, 11))
    row_block = jnp.arange(NLAT) // 150
    col_block = jnp.arange(NLON) // 64
    block_scales = jnp.exp(jax.random.uniform(scale_key, (NLAT // 150 + 1, NLON // 64 + 1), jnp.float32, math.log(0.1), math.log(3.0)))
    cell_scale = block_scales[row_block[:, None], col_block[None, :]]
    noise_values = jax.random.normal(noise_key, (NLAT, NLON), jnp.float32)
    return jnp.clip(noise_values * cell_scale, -8.0, 8.0)


def draw_land_sea(key, part):
    first_key, second_key, third_key = jax.random.split(jax.random.fold_in(key, 37), 3)
    band_count = NLON // 8
    continent = (jax.random.randint(first_key, (band_count,), 0, 3, jnp.int32) == 0) | (jnp.arange(band_count) == 0)
    start_row = jax.random.randint(second_key, (band_count,), 0, NLAT // 2, jnp.int32)
    extent = jax.random.randint(third_key, (band_count,), NLAT // 8 + 1, NLAT // 2 + 1, jnp.int32)
    band_of = jnp.arange(NLON, dtype=jnp.int32) // 8
    rows = jnp.arange(NLAT, dtype=jnp.int32)[:, None]
    land = continent[band_of][None, :] & (rows >= start_row[band_of][None, :]) & (rows < (start_row + extent)[band_of][None, :])
    return jnp.where(land, 0, 1).astype(jnp.int32)


def draw_fold_map(key, part):
    offset = 2 * jax.random.randint(jax.random.fold_in(key, 23), (), 0, NLON // 2, jnp.int32) + 1
    return (offset - jnp.arange(NLON, dtype=jnp.int32)) % NLON


def levels(rng, shape, cuts, low, top_value):
    factor_of = 1.0
    for dim, parts in cuts:
        draws = jax.random.uniform(jax.random.fold_in(jax.random.fold_in(rng, 6), dim), (parts,), jnp.float32, low / len(cuts), top_value / len(cuts))
        factor_of = factor_of * jnp.repeat(jnp.exp(draws), shape[dim] // parts).reshape((-1,) + (1,) * (len(shape) - 1 - dim))
    return factor_of


def setup_inputs(seed: int = 0) -> dict:
    keys = jax.random.split(jax.random.key(seed), 9)
    return {
        "right_side": draw_right_side(jax.random.fold_in(keys[8], 71), 0),
        "surface_term": jnp.clip(jnp.exp(math.log(0.002) - 2.3025852 * jax.random.uniform(keys[1], (NLAT, NLON), jnp.float32) ** levels(keys[1], (NLAT, NLON), ((0, 4), (1, 8)), -0.2, 0.2)), 0.0002, 0.002),
        "east_coupling": jnp.clip(jnp.exp(math.log(3.0) - 2.3025851 * jax.random.uniform(keys[2], (NLAT, NLON), jnp.float32) ** levels(keys[2], (NLAT, NLON), ((0, 4), (1, 8)), -0.2, 0.2)), 0.3, 3.0),
        "north_coupling": jnp.clip(jnp.exp(math.log(3.0) - 2.3025851 * jax.random.uniform(keys[3], (NLAT, NLON), jnp.float32) ** levels(keys[3], (NLAT, NLON), ((0, 4), (1, 8)), -0.2, 0.2)), 0.3, 3.0),
        "neast_coupling": jnp.clip(jnp.exp(math.log(0.5) - 1.609438 * jax.random.uniform(keys[4], (NLAT, NLON), jnp.float32) ** levels(keys[4], (NLAT, NLON), ((0, 4), (1, 8)), -0.2, 0.2)), 0.1, 0.5),
        "nwest_coupling": jnp.clip(jnp.exp(math.log(0.5) - 1.609438 * jax.random.uniform(keys[5], (NLAT, NLON), jnp.float32) ** levels(keys[5], (NLAT, NLON), ((0, 4), (1, 8)), -0.2, 0.2)), 0.1, 0.5),
        "land_sea": draw_land_sea(jax.random.fold_in(keys[8], 71), 0),
        "fold_map": draw_fold_map(jax.random.fold_in(keys[8], 71), 0),
    }


OFFSETS = ((0, 1), (0, -1), (1, 0), (-1, 0), (1, 1), (-1, -1), (1, -1), (-1, 1))
COUPLINGS = ((1, 0, 0), (1, 0, -1), (2, 0, 0), (2, -1, 0), (3, 0, 0), (3, -1, -1), (4, 0, 0), (4, -1, 1))

def interior(padded, row_step, col_step):
    row_count = padded.shape[-2] - 2
    col_count = padded.shape[-1] - 2
    return padded[..., 1 + row_step:1 + row_step + row_count, 1 + col_step:1 + col_step + col_count]

def stencil_weights(padded):
    ocean_pad = padded[0]
    centre = interior(ocean_pad, 0, 0)
    weight_list = []
    open_sum = jnp.zeros_like(centre)
    for (layer_index, row_step, col_step), (row_off, col_off) in zip(COUPLINGS, OFFSETS):
        edge_value = interior(padded[layer_index], row_step, col_step)
        weight_list.append(edge_value * centre * interior(ocean_pad, row_off, col_off))
        open_sum = open_sum + edge_value
    return (jnp.stack(weight_list), open_sum)

def neighbour_sum(weights, padded_field):
    accumulated = jnp.zeros_like(weights[0])
    for position, (row_off, col_off) in enumerate(OFFSETS):
        accumulated = accumulated + weights[position] * interior(padded_field, row_off, col_off)
    return accumulated

def pad_grid(values):
    wrapped = jnp.concatenate([values[..., -1:], values, values[..., :1]], axis=-1)
    zero_row = jnp.zeros_like(wrapped[..., :1, :])
    return jnp.concatenate([zero_row, wrapped, zero_row], axis=-2)

def line_solve(lower_band, middle_band, upper_band, values):
    solved = lax.linalg.tridiagonal_solve(lower_band.T, middle_band.T, upper_band.T, values.T[:, :, None])
    return solved[:, :, 0].T

def reference(right_side, surface_term, east_coupling, north_coupling, neast_coupling, nwest_coupling, land_sea, fold_map):
    ocean = land_sea.astype(jnp.float32)
    row_ids = lax.broadcasted_iota(jnp.int32, ocean.shape, 0)
    top_row = jnp.where(row_ids == ocean.shape[0] - 1, 1.0, 0.0).astype(jnp.float32)
    open_rows = 1.0 - top_row
    stacked = jnp.stack([ocean, east_coupling, north_coupling * open_rows, neast_coupling * open_rows, nwest_coupling * open_rows])
    weights, open_sum = stencil_weights(pad_grid(stacked))
    top_north = north_coupling[-1]
    fold_open = 0.5 * (top_north + jnp.take(top_north, fold_map))
    fold_weight = fold_open * ocean[-1] * jnp.take(ocean[-1], fold_map)
    diagonal = ocean * (surface_term + open_sum + top_row * fold_open[None]) + (1.0 - ocean)
    line_diagonal = ocean * (surface_term + weights[2] + weights[3]) + (1.0 - ocean)
    lower_band = -weights[3]
    upper_band = -weights[2]

    def operate(field):
        fold_term = fold_weight * jnp.take(field[-1], fold_map)
        return diagonal * field - neighbour_sum(weights, pad_grid(field)) - top_row * fold_term[None]
    residual = ocean * right_side
    solution = jnp.zeros_like(residual)
    precond = line_solve(lower_band, line_diagonal, upper_band, residual)
    direction = precond
    product_now = jnp.sum(residual * precond)
    for iteration in range(ITERS):
        image_field = operate(direction)
        step_length = product_now / jnp.sum(direction * image_field)
        solution = solution + step_length * direction
        residual = residual - step_length * image_field
        if iteration + 1 < ITERS:
            precond = line_solve(lower_band, line_diagonal, upper_band, residual)
            product_next = jnp.sum(residual * precond)
            direction = precond + product_next / product_now * direction
            product_now = product_next
    return (solution, residual)
```

```python
import functools

import jax
import jax.numpy as jnp
from jax import lax
from jax.experimental import pallas as pl
from jax.experimental.pallas import tpu as pltpu
from jax.sharding import PartitionSpec as P

ITERS = 8
SUB = 8


def iota(shape, dim):
    return lax.broadcasted_iota(jnp.int32, shape, dim)


def east(x):
    return pltpu.roll(x, x.shape[-1] - 1, x.ndim - 1)


def west(x):
    return pltpu.roll(x, 1, x.ndim - 1)


def from_above(x):
    return pltpu.roll(x, SUB - 1, 0)


def from_below(x):
    return pltpu.roll(x, 1, 0)


def kernel(
    lat_count,
    lon_count,
    shift_ref,
    right_ref,
    surface_ref,
    east_ref,
    north_ref,
    neast_ref,
    nwest_ref,
    land_ref,
    sol_out,
    res_out,
    w_e,
    w_w,
    w_n,
    w_s,
    w_ne,
    w_sw,
    w_nw,
    w_se,
    diag,
    f_a,
    f_g,
    resp0,
    resp1,
    u_ref,
    img,
    dirn,
    along,
    sol_ref,
    res_ref,
    fields,
    msg,
    recv,
    fold_ref,
    top_msg,
    top_recv,
    halo_msg,
    halo_recv,
    pack_msg,
    pack_recv,
    back_msg,
    back_recv,
    send_sem,
    recv_sem,
    top_send,
    top_arrive,
    halo_send,
    halo_arrive,
    pack_send,
    pack_arrive,
    back_send,
    back_arrive,
):
    n_dev = lat_count * lon_count
    lat = lax.axis_index("lat")
    lon = lax.axis_index("lon")
    me = lat * lon_count + lon
    depth, _, width = sol_ref.shape
    own = width // lat_count
    half = depth // 2
    top = depth - 1

    barrier = pltpu.get_barrier_semaphore()

    def greet(step, carry):
        peer = lax.rem(me + step, n_dev)
        pl.semaphore_signal(
            barrier,
            inc=1,
            device_id=(peer // lon_count, lax.rem(peer, lon_count)),
            device_id_type=pl.DeviceIdType.MESH,
        )
        return carry

    lax.fori_loop(1, n_dev, greet, 0, unroll=n_dev <= 64)

    lane = iota((1, width), 1)
    relative = lax.rem(lane - lat * own + width, width)
    own_row = relative < own

    def copy_to(parity, step):
        peer = lax.rem(me + step, n_dev)
        return pltpu.make_async_remote_copy(
            src_ref=msg.at[parity],
            dst_ref=recv.at[parity, me],
            send_sem=send_sem.at[parity, step],
            recv_sem=recv_sem.at[parity, step],
            device_id=(peer // lon_count, lax.rem(peer, lon_count)),
            device_id_type=pl.DeviceIdType.MESH,
        )

    def send_all(parity, row):
        msg[parity] = row
        recv[parity, me] = row

        def one(step, carry):
            copy_to(parity, step).start()
            return carry

        lax.fori_loop(1, n_dev, one, 0, unroll=n_dev <= 64)

    def wait_all(parity):
        def one(step, carry):
            copy_to(parity, step).wait()
            return carry

        lax.fori_loop(1, n_dev, one, 0, unroll=n_dev <= 64)
        top_row = jnp.zeros((lon_count, width), jnp.float32)
        rest = jnp.zeros((lon_count, width), jnp.float32)
        for place in range(lat_count):
            rows = jnp.concatenate(
                [recv[parity, place * lon_count + b] for b in range(lon_count)], axis=0
            )
            offset = lax.rem(iota((lon_count, width), 1) - place * own + width, width)
            top_row = top_row + jnp.where(offset < own, rows, 0.0)
            moved = pltpu.roll(rows, width - own, 1)
            rest = rest + jnp.where(offset < own, moved, 0.0)
        return top_row, rest

    mesh_id = pl.DeviceIdType.MESH
    rows = right_ref.shape[0]
    halo = ITERS
    span = own + 2 * halo
    pl.semaphore_wait(barrier, n_dev - 1)

    at_top = lat == lat_count - 1
    top_msg[0:1] = north_ref[rows - 1 :, :]
    top_msg[1:2] = land_ref[rows - 1 :, :].astype(jnp.float32)

    def top_copy(step):
        peer = lax.rem(me + step, n_dev)
        return pltpu.make_async_remote_copy(
            src_ref=top_msg,
            dst_ref=top_recv.at[lon],
            send_sem=top_send.at[step],
            recv_sem=top_arrive.at[lon],
            device_id=(peer // lon_count, lax.rem(peer, lon_count)),
            device_id_type=mesh_id,
        )

    @pl.when(at_top)
    def _():
        top_recv[lon] = top_msg[...]

        def one(step, carry):
            top_copy(step).start()
            return carry

        lax.fori_loop(1, n_dev, one, 0, unroll=n_dev <= 64)

    given = (right_ref, surface_ref, east_ref, north_ref, neast_ref, nwest_ref, land_ref)
    count = len(given)

    def local(index, v):
        return given[index][v * SUB : (v + 1) * SUB, :].astype(jnp.float32)

    wide = iota((SUB, width), 1)

    def halo_copy(side):
        step = lon_count - 1 if side else 1
        return pltpu.make_async_remote_copy(
            src_ref=halo_msg.at[side],
            dst_ref=halo_recv.at[side],
            send_sem=halo_send.at[side],
            recv_sem=halo_arrive.at[side],
            device_id=(lat, lax.rem(lon + step, lon_count)),
            device_id_type=mesh_id,
        )

    for v in range(rows // SUB):
        eastward = jnp.zeros((SUB, width), jnp.float32)
        westward = eastward
        for i in range(count):
            turned = pltpu.roll(local(i, v), halo * (i + 1), 1)
            slot = wide // halo
            eastward = jnp.where(slot == i, turned, eastward)
            westward = jnp.where(slot == i + 1, turned, westward)
        halo_msg[0, v * SUB : (v + 1) * SUB] = eastward
        halo_msg[1, v * SUB : (v + 1) * SUB] = westward
    halo_copy(0).start()
    halo_copy(1).start()

    def pack(place):
        for v in range(rows // SUB):
            sl = slice(v * SUB, (v + 1) * SUB)
            values = [local(i, v) for i in range(count)]

            def window(i, shift):
                out = pltpu.roll(values[i], (shift - (place * own - halo)) % width, 1)
                if place == 0:
                    left = pltpu.roll(halo_recv[0, sl], (shift - halo * i) % width, 1)
                    out = jnp.where((wide >= shift) & (wide < shift + halo), left, out)
                if place == lat_count - 1:
                    low = shift + halo + own
                    right = pltpu.roll(halo_recv[1, sl], (low - halo * (i + 1)) % width, 1)
                    out = jnp.where((wide >= low) & (wide < low + halo), right, out)
                return out

            first, second = wide < span, wide < 2 * span
            third = wide < 2 * span + halo
            pack_msg[place, 0, sl] = jnp.where(
                first, window(0, 0), jnp.where(second, window(1, span), window(6, 2 * span - halo))
            )
            edge = jnp.where(third, window(6, 2 * span), window(6, 2 * span - own))
            pack_msg[place, 1, sl] = jnp.where(
                first, window(2, 0), jnp.where(second, window(3, span), edge)
            )
            pack_msg[place, 2, sl] = jnp.where(first, window(4, 0), window(5, span))

    here = pl.ds(pl.multiple_of(lat * rows, rows), rows)

    def pack_copy(place):
        return pltpu.make_async_remote_copy(
            src_ref=pack_msg.at[place],
            dst_ref=pack_recv.at[:, here],
            send_sem=pack_send.at[place],
            recv_sem=pack_arrive.at[lat],
            device_id=(place, lon),
            device_id_type=mesh_id,
        )

    for place in [*range(1, lat_count - 1), 0, lat_count - 1]:
        if place == 0:
            halo_copy(0).wait()
            halo_copy(1).wait()
        pack(place)

        @pl.when(lat != place)
        def _(place=place):
            pack_copy(place).start()

    pack_recv[:, here] = pack_msg[lat]
    for place in range(lat_count):

        @pl.when(lat != place)
        def _(place=place):
            pack_copy(place).wait_send()
            pltpu.make_async_remote_copy(
                src_ref=pack_msg.at[place],
                dst_ref=pack_recv.at[:, place * rows : (place + 1) * rows],
                send_sem=pack_send.at[place],
                recv_sem=pack_arrive.at[place],
                device_id=(place, lon),
                device_id_type=mesh_id,
            ).wait_recv()

    start = lat * own - halo + 2 * width
    offset8 = lax.rem(wide - lat * own + halo + width, width)
    inside = offset8 < span
    own8 = (offset8 >= halo) & (offset8 < halo + own)
    for k in range(depth):
        packed = [pack_recv[c, pl.ds(k, SUB, stride=depth), :] for c in range(3)]

        def place_at(c, slot):
            return pltpu.roll(packed[c], lax.rem(start - slot, width), 1)

        mask = jnp.where(offset8 < halo, place_at(1, 2 * span), place_at(1, 2 * span - own))
        mask = jnp.where(own8, place_at(0, 2 * span - halo), mask)
        fields[6, k] = jnp.where(inside, mask, 0.0)
        for i in range(6):
            fields[i, k] = jnp.where(inside, place_at(i // 2, span * (i % 2)), 0.0)

    def field(index, k):
        return fields[index, k]

    is_top = iota((SUB, width), 0) == SUB - 1

    def closed(index, k):
        value = field(index, k)
        return jnp.where(is_top, 0.0, value) if k == top else value

    def above(index, k):
        return field(index, k + 1) if k < top else from_above(field(index, 0))

    n_prev, ne_prev, nw_prev = (from_below(closed(i, top)) for i in (3, 4, 5))
    for k in range(depth):
        ocean = field(6, k)
        ocean_north = above(6, k)
        e_now, n_now, ne_now, nw_now = field(2, k), closed(3, k), closed(4, k), closed(5, k)
        we = e_now * ocean * east(ocean)
        wn = n_now * ocean * ocean_north
        wne = ne_now * ocean * east(ocean_north)
        wnw = nw_now * ocean * west(ocean_north)
        w_e[k] = we
        w_w[k] = west(we)
        w_n[k] = wn
        w_ne[k] = wne
        w_nw[k] = wnw
        sw, se = west(wne), east(wnw)
        if k < top:
            w_s[k + 1] = wn
            w_sw[k + 1] = sw
            w_se[k + 1] = se
        else:
            w_s[0] = from_below(wn)
            w_sw[0] = from_below(sw)
            w_se[0] = from_below(se)
        open_sum = (
            e_now + west(e_now) + n_now + n_prev + ne_now + west(ne_prev) + nw_now + east(nw_prev)
        )
        diag[k] = ocean * (field(1, k) + open_sum) + (1.0 - ocean)
        n_prev, ne_prev, nw_prev = n_now, ne_now, nw_now
        res_ref[k] = ocean * field(0, k)
        sol_ref[k] = jnp.zeros((SUB, width), jnp.float32)
        dirn[k] = jnp.zeros((SUB, width), jnp.float32)
        along[k] = jnp.zeros((SUB, width), jnp.float32)

    def surface(k):
        ocean = field(6, k)
        return ocean * field(1, k) + (1.0 - ocean)

    low = surface(0) + w_s[0]
    high = surface(top) + w_n[top]
    for k in range(half):
        up, j = k, top - k
        g_low = 1.0 / (low + w_n[up])
        g_high = 1.0 / (high + w_s[j])
        f_g[up] = g_low
        f_g[j] = g_high
        if k < half - 1:
            f_a[up + 1] = w_n[up] * g_low
            f_a[j - 1] = w_s[j] * g_high
            low = surface(up + 1) + w_n[up] * (low * g_low)
            high = surface(j - 1) + w_s[j] * (high * g_high)
    mid = w_n[half - 1]
    inv_det = 1.0 / (low * high + mid * (low + high))
    mid_ll = (high + mid) * inv_det
    mid_lh = mid * inv_det
    mid_hh = (low + mid) * inv_det

    def line(read, write):
        y, z = read(0), read(top)
        ys, zs = [y], [z]
        u_ref[0] = y
        u_ref[top] = z
        for k in range(1, half):
            j = top - k
            y = read(k) + f_a[k] * y
            z = read(j) + f_a[j] * z
            u_ref[k] = y
            u_ref[j] = z
        x = mid_ll * y + mid_lh * z
        v = mid_lh * y + mid_hh * z
        write(half - 1, x)
        write(half, v)
        for k in range(half - 2, -1, -1):
            j = top - k
            x = f_g[k] * u_ref[k] + f_a[k + 1] * x
            v = f_g[j] * u_ref[j] + f_a[j - 1] * v
            write(k, x)
            write(j, v)

    zero = jnp.zeros((SUB, width), jnp.float32)
    line(lambda k: w_s[0] if k == 0 else zero, lambda k, v: resp0.__setitem__(k, v))
    line(lambda k: w_n[top] if k == top else zero, lambda k, v: resp1.__setitem__(k, v))

    a, b, c, d = resp0[0], resp1[0], resp0[top], resp1[top]
    plan = []
    stride = 1
    while stride < SUB:
        def below(x, stride=stride):
            return pltpu.roll(x, stride, 0)

        def over(x, stride=stride):
            return pltpu.roll(x, SUB - stride, 0)

        cb, db = below(c), below(d)
        aa, ba = over(a), over(b)
        m00, m01 = 1.0 - a * db, -b * aa
        m10, m11 = -c * db, 1.0 - d * aa
        inv = 1.0 / (m00 * m11 - m01 * m10)
        i00, i01, i10, i11 = m11 * inv, -m01 * inv, -m10 * inv, m00 * inv
        t0, t1 = i00 * a + i01 * c, i00 * b + i01 * d
        t2, t3 = i10 * a + i11 * c, i10 * b + i11 * d
        plan.append((stride, i00, i01, i10, i11, t0, t1, t2, t3))
        a, b, c, d = t0 * cb, t1 * ba, t2 * cb, t3 * ba
        stride *= 2

    def interface(p, q):
        for stride, i00, i01, i10, i11, t0, t1, t2, t3 in plan:
            qb = pltpu.roll(q, stride, 0)
            pa = pltpu.roll(p, SUB - stride, 0)
            p, q = (
                (i00 * p + i01 * q) + (t0 * qb + t1 * pa),
                (i10 * p + i11 * q) + (t2 * qb + t3 * pa),
            )
        return from_below(q), from_above(p)

    @pl.when(at_top)
    def _():
        def one(step, carry):
            top_copy(step).wait_send()
            return carry

        lax.fori_loop(1, n_dev, one, 0, unroll=n_dev <= 64)

    for b in range(lon_count):

        @pl.when(jnp.logical_or(lat != lat_count - 1, lon != b))
        def _(b=b):
            pltpu.make_async_remote_copy(
                src_ref=top_msg,
                dst_ref=top_recv.at[b],
                send_sem=top_send.at[0],
                recv_sem=top_arrive.at[b],
                device_id=(lat_count - 1, b),
                device_id_type=mesh_id,
            ).wait_recv()

    whole_north = jnp.concatenate([top_recv[b][0:1] for b in range(lon_count)], axis=0)
    whole_ocean = jnp.concatenate([top_recv[b][1:2] for b in range(lon_count)], axis=0)
    total_cols = lon_count * width
    back = total_cols - 1 - shift_ref[0]
    row_shift = back // width
    lane_shift = lax.rem(back, width)
    lanes = iota((lon_count, width), 1)

    def facing(rows):
        flipped = jnp.concatenate(
            [rows[b : b + 1] for b in range(lon_count - 1, -1, -1)], axis=0
        )
        index = width - 1 - lax.rem(lanes + lane_shift, width)
        turned = jnp.take_along_axis(flipped, index, axis=1)
        first = pltpu.roll(turned, lax.rem(lon_count - row_shift, lon_count), 0)
        second = pltpu.roll(turned, lon_count - 1 - row_shift, 0)
        return jnp.where(lanes + lane_shift < width, first, second)

    fold_open = 0.5 * (whole_north + facing(whole_north))
    fold_ref[0] = fold_open * whole_ocean
    fold_ref[1] = fold_open * whole_ocean * facing(whole_ocean)
    rows_id = iota((lon_count, width), 0)
    reach = lax.rem(lanes - lat * own + width + (width - own) // 2, width) - (width - own) // 2
    spill = lat * own + reach
    home = jnp.where(spill < 0, -1, jnp.where(spill >= width, 1, 0))
    pick = rows_id == lax.rem(lon + home + lon_count, lon_count)

    def iterate(step, carry):
        rz_old, step_old = carry
        parity = lax.rem(step, 2)
        line(lambda k: res_ref[k], lambda k, v: u_ref.__setitem__(k, v))
        below, over = interface(u_ref[0], u_ref[top])
        accs = [zero, zero, zero, zero]

        def finish(k):
            value = u_ref[k] + below * resp0[k] + over * resp1[k]
            u_ref[k] = value
            accs[k % 2] = accs[k % 2] + res_ref[k] * value
            return (value, east(value), west(value))

        last = finish(top)
        first = finish(0)
        prev = tuple(from_below(x) for x in last)
        now = first
        for k in range(depth):
            if k < top - 1:
                nxt = finish(k + 1)
            elif k == top - 1:
                nxt = last
            else:
                nxt = tuple(from_above(x) for x in first)
            value = (
                (diag[k] * now[0] - w_e[k] * now[1] - w_w[k] * now[2])
                - (w_n[k] * nxt[0] + w_ne[k] * nxt[1] + w_nw[k] * nxt[2])
                - (w_s[k] * prev[0] + w_se[k] * prev[1] + w_sw[k] * prev[2])
            )
            img[k] = value
            accs[2 + k % 2] = accs[2 + k % 2] + now[0] * value
            prev, now = now, nxt
        rz_part = jnp.sum(jnp.where(own_row, accs[0] + accs[1], 0.0), keepdims=True)
        curve_part = jnp.sum(jnp.where(own_row, accs[2] + accs[3], 0.0), keepdims=True)
        row = jnp.where(own_row, last[0][SUB - 1 :], 0.0)
        row = jnp.where(relative == own, rz_part, row)
        row = jnp.where(relative == own + 1, curve_part, row)
        send_all(parity, row)
        top_row, rest = wait_all(parity)
        rest_lane = lax.rem(lanes, own)
        fold_image = fold_ref[0] * top_row - fold_ref[1] * facing(top_row)
        rz = jnp.sum(jnp.where(rest_lane == 0, rest, 0.0), keepdims=True)
        curve = jnp.sum(
            jnp.where(rest_lane == 1, rest, 0.0) + fold_image * top_row, keepdims=True
        )
        fix = jnp.sum(jnp.where(pick, fold_image, 0.0), axis=0, keepdims=True)
        img[top] = img[top] + jnp.where(is_top, fix, 0.0)
        ratio = jnp.where(step == 0, 0.0, rz / rz_old)
        length = rz / (curve - ratio * rz / step_old)
        ratio_v = jnp.broadcast_to(ratio, (SUB, width))
        length_v = jnp.broadcast_to(length, (SUB, width))
        for k in range(depth):
            toward = u_ref[k] + ratio_v * dirn[k]
            moved = img[k] + ratio_v * along[k]
            dirn[k] = toward
            along[k] = moved
            sol_ref[k] = sol_ref[k] + length_v * toward
            res_ref[k] = res_ref[k] - length_v * moved
        return (rz, length)

    one = jnp.ones((1, 1), jnp.float32)
    lax.fori_loop(0, ITERS, iterate, (one, one))

    quarter = depth // 2
    place8 = lax.rem(wide - lat * own + width, width)
    for k in range(quarter):
        row = jnp.where(place8 < own, sol_ref[k], pltpu.roll(res_ref[k], own, 1))
        later = jnp.where(
            place8 < 3 * own,
            pltpu.roll(sol_ref[k + quarter], 2 * own, 1),
            pltpu.roll(res_ref[k + quarter], 3 * own, 1),
        )
        back_msg[pl.ds(k, SUB, stride=quarter), :] = jnp.where(place8 < 2 * own, row, later)
    part = rows // 2

    def back_copy(place):
        return pltpu.make_async_remote_copy(
            src_ref=back_msg.at[place * part : (place + 1) * part],
            dst_ref=back_recv.at[lat],
            send_sem=back_send.at[place],
            recv_sem=back_arrive.at[lat],
            device_id=(place, lon),
            device_id_type=mesh_id,
        )

    for place in range(lat_count):

        @pl.when(lat != place)
        def _(place=place):
            back_copy(place).start()

    back_recv[lat] = back_msg[pl.ds(pl.multiple_of(lat * part, part), part), :]
    for place in range(lat_count):

        @pl.when(lat != place)
        def _(place=place):
            back_copy(place).wait_send()
            pltpu.make_async_remote_copy(
                src_ref=back_msg.at[place * part : (place + 1) * part],
                dst_ref=back_recv.at[place],
                send_sem=back_send.at[place],
                recv_sem=back_arrive.at[place],
                device_id=(place, lon),
                device_id_type=mesh_id,
            ).wait_recv()

    for v in range(part // SUB):
        block, k = divmod(v * SUB, quarter)
        parts = [jnp.zeros((SUB, width), jnp.float32)] * 4
        for place in range(lat_count):
            piece = back_recv[place, v * SUB : (v + 1) * SUB]
            mine = (wide >= place * own) & (wide < (place + 1) * own)
            for i in range(4):
                moved = pltpu.roll(piece, (width - i * own) % width, 1) if i else piece
                parts[i] = jnp.where(mine, moved, parts[i])
        low = block * depth + k
        sol_out[low : low + SUB] = parts[0]
        res_out[low : low + SUB] = parts[1]
        sol_out[low + quarter : low + quarter + SUB] = parts[2]
        res_out[low + quarter : low + quarter + SUB] = parts[3]


def shards(
    right_side,
    surface_term,
    east_coupling,
    north_coupling,
    neast_coupling,
    nwest_coupling,
    land_sea,
    fold_map,
):
    rows, width = right_side.shape
    lat_count = lax.axis_size("lat")
    lon_count = lax.axis_size("lon")
    lon = lax.axis_index("lon")
    n_dev = lat_count * lon_count
    depth = rows * lat_count // SUB
    columns = lon_count * width
    turn = lax.rem(fold_map[:1] + lon * width, columns)

    block = pltpu.VMEM((depth, SUB, width), jnp.float32)
    answer = jax.ShapeDtypeStruct((rows, width), jnp.float32)
    vmem = pl.BlockSpec(memory_space=pltpu.VMEM)
    dma = pltpu.SemaphoreType.DMA

    def held(*shape):
        return pltpu.VMEM((*shape, width), jnp.float32)

    return pl.pallas_call(
        functools.partial(kernel, lat_count, lon_count),
        out_shape=(answer, answer),
        in_specs=[pl.BlockSpec(memory_space=pltpu.SMEM)] + [vmem] * 7,
        out_specs=(vmem, vmem),
        scratch_shapes=[block] * 19
        + [
            held(7, depth, SUB),
            held(2, 1),
            held(2, n_dev, 1),
            held(2, lon_count),
            held(2),
            held(lon_count, 2),
            held(2, rows),
            held(2, rows),
            held(lat_count, 3, rows),
            held(3, lat_count * rows),
            held(lat_count * rows // 2),
            held(lat_count, rows // 2),
            dma((2, n_dev)),
            dma((2, n_dev)),
            dma((n_dev,)),
            dma((lon_count,)),
            dma((2,)),
            dma((2,)),
            dma((lat_count,)),
            dma((lat_count,)),
            dma((lat_count,)),
            dma((lat_count,)),
        ],
        compiler_params=pltpu.CompilerParams(collective_id=0, has_side_effects=True),
    )(
        turn,
        right_side,
        surface_term,
        east_coupling,
        north_coupling,
        neast_coupling,
        nwest_coupling,
        land_sea,
    )


def solution(mesh):
    return jax.shard_map(
        shards,
        mesh=mesh,
        in_specs=(P("lat", "lon"),) * 7 + (P("lon"),),
        out_specs=(P("lat", "lon"), P("lat", "lon")),
        check_vma=False,
    )
```

```python
import functools

import jax
import jax.numpy as jnp
from jax import lax
from jax.experimental import pallas as pl
from jax.experimental.pallas import tpu as pltpu
from jax.sharding import PartitionSpec as P

ITERS = 8
SUB = 8


def iota(shape, dim):
    return lax.broadcasted_iota(jnp.int32, shape, dim)


def east(x):
    return pltpu.roll(x, x.shape[-1] - 1, x.ndim - 1)


def west(x):
    return pltpu.roll(x, 1, x.ndim - 1)


def from_above(x):
    return pltpu.roll(x, SUB - 1, 0)


def from_below(x):
    return pltpu.roll(x, 1, 0)


def kernel(
    lat_count,
    lon_count,
    shift_ref,
    right_ref,
    surface_ref,
    east_ref,
    north_ref,
    neast_ref,
    nwest_ref,
    land_ref,
    sol_out,
    res_out,
    w_e,
    w_w,
    w_n,
    w_s,
    w_ne,
    w_sw,
    w_nw,
    w_se,
    diag,
    f_a,
    f_g,
    resp0,
    resp1,
    u_pair,
    img,
    dirn,
    along,
    sol_ref,
    res_ref,
    fields,
    msg,
    recv,
    fold_ref,
    top_msg,
    top_recv,
    halo_msg,
    halo_recv,
    pack_msg,
    pack_recv,
    back_msg,
    back_recv,
    send_sem,
    recv_sem,
    top_send,
    top_arrive,
    halo_send,
    halo_arrive,
    pack_send,
    pack_arrive,
    back_send,
    back_arrive,
):
    n_dev = lat_count * lon_count
    lat = lax.axis_index("lat")
    lon = lax.axis_index("lon")
    me = lat * lon_count + lon
    depth, _, width = sol_ref.shape
    own = width // lat_count
    half = depth // 2
    top = depth - 1

    barrier = pltpu.get_barrier_semaphore()

    def greet(step, carry):
        peer = lax.rem(me + step, n_dev)
        pl.semaphore_signal(
            barrier,
            inc=1,
            device_id=(peer // lon_count, lax.rem(peer, lon_count)),
            device_id_type=pl.DeviceIdType.MESH,
        )
        return carry

    lax.fori_loop(1, n_dev, greet, 0, unroll=n_dev <= 64)

    lane = iota((1, width), 1)
    relative = lax.rem(lane - lat * own + width, width)
    own_row = relative < own

    def alternate(size):
        ring = []
        for i in range(1, size // 2 + 1):
            ring += [size - i, i]
        return list(dict.fromkeys([*ring, 0]))

    lats = {d: lax.rem(lat + d, lat_count) for d in range(lat_count)}
    lons = {d: lax.rem(lon + d, lon_count) for d in range(lon_count)}
    peers = [(p, q) for q in alternate(lon_count) for p in alternate(lat_count) if p or q]

    def copy_to(parity, place):
        return pltpu.make_async_remote_copy(
            src_ref=msg.at[parity],
            dst_ref=recv.at[parity, me],
            send_sem=send_sem.at[parity],
            recv_sem=recv_sem.at[parity],
            device_id=place,
            device_id_type=pl.DeviceIdType.MESH,
        )

    def send_all(parity, row):
        msg[parity] = row
        recv[parity, me] = row
        if n_dev <= 64:
            for p, q in peers:
                copy_to(parity, (lats[p], lons[q])).start()
            return

        def one(step, carry):
            peer = lax.rem(me + step, n_dev)
            copy_to(parity, (peer // lon_count, lax.rem(peer, lon_count))).start()
            return carry

        lax.fori_loop(1, n_dev, one, 0)

    def wait_all(parity):
        every = recv.at[parity, 0 : n_dev - 1]
        pltpu.make_async_remote_copy(
            src_ref=every,
            dst_ref=every,
            send_sem=send_sem.at[parity],
            recv_sem=recv_sem.at[parity],
            device_id=(lats[0], lons[1]),
            device_id_type=pl.DeviceIdType.MESH,
        ).wait()
        top_row = jnp.zeros((lon_count, width), jnp.float32)
        rest = jnp.zeros((lon_count, width), jnp.float32)
        for place in range(lat_count):
            rows = jnp.concatenate(
                [recv[parity, place * lon_count + b] for b in range(lon_count)], axis=0
            )
            offset = lax.rem(iota((lon_count, width), 1) - place * own + width, width)
            top_row = top_row + jnp.where(offset < own, rows, 0.0)
            moved = pltpu.roll(rows, width - own, 1)
            rest = rest + jnp.where(offset < own, moved, 0.0)
        return top_row, rest

    mesh_id = pl.DeviceIdType.MESH
    rows = right_ref.shape[0]
    halo = ITERS
    span = own + 2 * halo
    pl.semaphore_wait(barrier, n_dev - 1)

    at_top = lat == lat_count - 1
    top_msg[0:1] = north_ref[rows - 1 :, :]
    top_msg[1:2] = land_ref[rows - 1 :, :].astype(jnp.float32)

    def top_copy(step):
        peer = lax.rem(me + step, n_dev)
        return pltpu.make_async_remote_copy(
            src_ref=top_msg,
            dst_ref=top_recv.at[lon],
            send_sem=top_send.at[step],
            recv_sem=top_arrive.at[lon],
            device_id=(peer // lon_count, lax.rem(peer, lon_count)),
            device_id_type=mesh_id,
        )

    @pl.when(at_top)
    def _():
        top_recv[lon] = top_msg[...]

        def one(step, carry):
            top_copy(step).start()
            return carry

        lax.fori_loop(1, n_dev, one, 0, unroll=n_dev <= 64)

    given = (right_ref, surface_ref, east_ref, north_ref, neast_ref, nwest_ref, land_ref)
    count = len(given)

    def local(index, v):
        return given[index][v * SUB : (v + 1) * SUB, :].astype(jnp.float32)

    wide = iota((SUB, width), 1)

    def halo_copy(side):
        step = lon_count - 1 if side else 1
        return pltpu.make_async_remote_copy(
            src_ref=halo_msg.at[side],
            dst_ref=halo_recv.at[side],
            send_sem=halo_send.at[side],
            recv_sem=halo_arrive.at[side],
            device_id=(lat, lax.rem(lon + step, lon_count)),
            device_id_type=mesh_id,
        )

    for v in range(rows // SUB):
        eastward = jnp.zeros((SUB, width), jnp.float32)
        westward = eastward
        for i in range(count):
            turned = pltpu.roll(local(i, v), halo * (i + 1), 1)
            slot = wide // halo
            eastward = jnp.where(slot == i, turned, eastward)
            westward = jnp.where(slot == i + 1, turned, westward)
        halo_msg[0, v * SUB : (v + 1) * SUB] = eastward
        halo_msg[1, v * SUB : (v + 1) * SUB] = westward
    halo_copy(0).start()
    halo_copy(1).start()

    def pack(place):
        for v in range(rows // SUB):
            sl = slice(v * SUB, (v + 1) * SUB)
            values = [local(i, v) for i in range(count)]

            def window(i, shift):
                out = pltpu.roll(values[i], (shift - (place * own - halo)) % width, 1)
                if place == 0:
                    left = pltpu.roll(halo_recv[0, sl], (shift - halo * i) % width, 1)
                    out = jnp.where((wide >= shift) & (wide < shift + halo), left, out)
                if place == lat_count - 1:
                    low = shift + halo + own
                    right = pltpu.roll(halo_recv[1, sl], (low - halo * (i + 1)) % width, 1)
                    out = jnp.where((wide >= low) & (wide < low + halo), right, out)
                return out

            first, second = wide < span, wide < 2 * span
            third = wide < 2 * span + halo
            pack_msg[place, 0, sl] = jnp.where(
                first, window(0, 0), jnp.where(second, window(1, span), window(6, 2 * span - halo))
            )
            edge = jnp.where(third, window(6, 2 * span), window(6, 2 * span - own))
            pack_msg[place, 1, sl] = jnp.where(
                first, window(2, 0), jnp.where(second, window(3, span), edge)
            )
            pack_msg[place, 2, sl] = jnp.where(first, window(4, 0), window(5, span))

    here = pl.ds(pl.multiple_of(lat * rows, rows), rows)

    def pack_copy(place):
        return pltpu.make_async_remote_copy(
            src_ref=pack_msg.at[place],
            dst_ref=pack_recv.at[:, here],
            send_sem=pack_send.at[place],
            recv_sem=pack_arrive.at[lat],
            device_id=(place, lon),
            device_id_type=mesh_id,
        )

    for place in [*range(1, lat_count - 1), 0, lat_count - 1]:
        if place == 0:
            halo_copy(0).wait()
            halo_copy(1).wait()
        pack(place)

        @pl.when(lat != place)
        def _(place=place):
            pack_copy(place).start()

    pack_recv[:, here] = pack_msg[lat]
    for place in range(lat_count):

        @pl.when(lat != place)
        def _(place=place):
            pack_copy(place).wait_send()
            pltpu.make_async_remote_copy(
                src_ref=pack_msg.at[place],
                dst_ref=pack_recv.at[:, place * rows : (place + 1) * rows],
                send_sem=pack_send.at[place],
                recv_sem=pack_arrive.at[place],
                device_id=(place, lon),
                device_id_type=mesh_id,
            ).wait_recv()

    start = lat * own - halo + 2 * width
    offset8 = lax.rem(wide - lat * own + halo + width, width)
    inside = offset8 < span
    own8 = (offset8 >= halo) & (offset8 < halo + own)
    for k in range(depth):
        packed = [pack_recv[c, pl.ds(k, SUB, stride=depth), :] for c in range(3)]

        def place_at(c, slot):
            return pltpu.roll(packed[c], lax.rem(start - slot, width), 1)

        mask = jnp.where(offset8 < halo, place_at(1, 2 * span), place_at(1, 2 * span - own))
        mask = jnp.where(own8, place_at(0, 2 * span - halo), mask)
        fields[6, k] = jnp.where(inside, mask, 0.0)
        for i in range(6):
            fields[i, k] = jnp.where(inside, place_at(i // 2, span * (i % 2)), 0.0)

    def field(index, k):
        return fields[index, k]

    is_top = iota((SUB, width), 0) == SUB - 1

    def closed(index, k):
        value = field(index, k)
        return jnp.where(is_top, 0.0, value) if k == top else value

    def above(index, k):
        return field(index, k + 1) if k < top else from_above(field(index, 0))

    n_prev, ne_prev, nw_prev = (from_below(closed(i, top)) for i in (3, 4, 5))
    for k in range(depth):
        ocean = field(6, k)
        ocean_north = above(6, k)
        e_now, n_now, ne_now, nw_now = field(2, k), closed(3, k), closed(4, k), closed(5, k)
        we = e_now * ocean * east(ocean)
        wn = n_now * ocean * ocean_north
        wne = ne_now * ocean * east(ocean_north)
        wnw = nw_now * ocean * west(ocean_north)
        w_e[k] = we
        w_w[k] = west(we)
        w_n[k] = wn
        w_ne[k] = wne
        w_nw[k] = wnw
        sw, se = west(wne), east(wnw)
        if k < top:
            w_s[k + 1] = wn
            w_sw[k + 1] = sw
            w_se[k + 1] = se
        else:
            w_s[0] = from_below(wn)
            w_sw[0] = from_below(sw)
            w_se[0] = from_below(se)
        open_sum = (
            e_now + west(e_now) + n_now + n_prev + ne_now + west(ne_prev) + nw_now + east(nw_prev)
        )
        diag[k] = ocean * (field(1, k) + open_sum) + (1.0 - ocean)
        n_prev, ne_prev, nw_prev = n_now, ne_now, nw_now
        res_ref[k] = ocean * field(0, k)
        sol_ref[k] = jnp.zeros((SUB, width), jnp.float32)
        dirn[k] = jnp.zeros((SUB, width), jnp.float32)
        along[k] = jnp.zeros((SUB, width), jnp.float32)

    def surface(k):
        ocean = field(6, k)
        return ocean * field(1, k) + (1.0 - ocean)

    low = surface(0) + w_s[0]
    high = surface(top) + w_n[top]
    for k in range(half):
        up, j = k, top - k
        g_low = 1.0 / (low + w_n[up])
        g_high = 1.0 / (high + w_s[j])
        f_g[up] = g_low
        f_g[j] = g_high
        if k < half - 1:
            f_a[up + 1] = w_n[up] * g_low
            f_a[j - 1] = w_s[j] * g_high
            low = surface(up + 1) + w_n[up] * (low * g_low)
            high = surface(j - 1) + w_s[j] * (high * g_high)
    mid = w_n[half - 1]
    inv_det = 1.0 / (low * high + mid * (low + high))
    mid_ll = (high + mid) * inv_det
    mid_lh = mid * inv_det
    mid_hh = (low + mid) * inv_det

    def line(read, write, u_ref=u_pair.at[0]):
        y, z = read(0), read(top)
        ys, zs = [y], [z]
        u_ref[0] = y
        u_ref[top] = z
        for k in range(1, half):
            j = top - k
            y = read(k) + f_a[k] * y
            z = read(j) + f_a[j] * z
            u_ref[k] = y
            u_ref[j] = z
        x = mid_ll * y + mid_lh * z
        v = mid_lh * y + mid_hh * z
        write(half - 1, x)
        write(half, v)
        for k in range(half - 2, -1, -1):
            j = top - k
            x = f_g[k] * u_ref[k] + f_a[k + 1] * x
            v = f_g[j] * u_ref[j] + f_a[j - 1] * v
            write(k, x)
            write(j, v)

    zero = jnp.zeros((SUB, width), jnp.float32)
    line(lambda k: w_s[0] if k == 0 else zero, lambda k, v: resp0.__setitem__(k, v))
    line(lambda k: w_n[top] if k == top else zero, lambda k, v: resp1.__setitem__(k, v))

    a, b, c, d = resp0[0], resp1[0], resp0[top], resp1[top]
    plan = []
    stride = 1
    while stride < SUB:
        def below(x, stride=stride):
            return pltpu.roll(x, stride, 0)

        def over(x, stride=stride):
            return pltpu.roll(x, SUB - stride, 0)

        cb, db = below(c), below(d)
        aa, ba = over(a), over(b)
        m00, m01 = 1.0 - a * db, -b * aa
        m10, m11 = -c * db, 1.0 - d * aa
        inv = 1.0 / (m00 * m11 - m01 * m10)
        i00, i01, i10, i11 = m11 * inv, -m01 * inv, -m10 * inv, m00 * inv
        t0, t1 = i00 * a + i01 * c, i00 * b + i01 * d
        t2, t3 = i10 * a + i11 * c, i10 * b + i11 * d
        plan.append((stride, i00, i01, i10, i11, t0, t1, t2, t3))
        a, b, c, d = t0 * cb, t1 * ba, t2 * cb, t3 * ba
        stride *= 2

    def interface(p, q):
        for stride, i00, i01, i10, i11, t0, t1, t2, t3 in plan:
            qb = pltpu.roll(q, stride, 0)
            pa = pltpu.roll(p, SUB - stride, 0)
            p, q = (
                (i00 * p + i01 * q) + (t0 * qb + t1 * pa),
                (i10 * p + i11 * q) + (t2 * qb + t3 * pa),
            )
        return from_below(q), from_above(p)

    @pl.when(at_top)
    def _():
        def one(step, carry):
            top_copy(step).wait_send()
            return carry

        lax.fori_loop(1, n_dev, one, 0, unroll=n_dev <= 64)

    for b in range(lon_count):

        @pl.when(jnp.logical_or(lat != lat_count - 1, lon != b))
        def _(b=b):
            pltpu.make_async_remote_copy(
                src_ref=top_msg,
                dst_ref=top_recv.at[b],
                send_sem=top_send.at[0],
                recv_sem=top_arrive.at[b],
                device_id=(lat_count - 1, b),
                device_id_type=mesh_id,
            ).wait_recv()

    whole_north = jnp.concatenate([top_recv[b][0:1] for b in range(lon_count)], axis=0)
    whole_ocean = jnp.concatenate([top_recv[b][1:2] for b in range(lon_count)], axis=0)
    total_cols = lon_count * width
    back = total_cols - 1 - shift_ref[0]
    row_shift = back // width
    lane_shift = lax.rem(back, width)
    lanes = iota((lon_count, width), 1)

    def facing(rows):
        flipped = jnp.concatenate(
            [rows[b : b + 1] for b in range(lon_count - 1, -1, -1)], axis=0
        )
        index = width - 1 - lax.rem(lanes + lane_shift, width)
        turned = jnp.take_along_axis(flipped, index, axis=1)
        first = pltpu.roll(turned, lax.rem(lon_count - row_shift, lon_count), 0)
        second = pltpu.roll(turned, lon_count - 1 - row_shift, 0)
        return jnp.where(lanes + lane_shift < width, first, second)

    fold_open = 0.5 * (whole_north + facing(whole_north))
    fold_ref[0] = fold_open * whole_ocean
    fold_ref[1] = fold_open * whole_ocean * facing(whole_ocean)
    rows_id = iota((lon_count, width), 0)
    reach = lax.rem(lanes - lat * own + width + (width - own) // 2, width) - (width - own) // 2
    spill = lat * own + reach
    home = jnp.where(spill < 0, -1, jnp.where(spill >= width, 1, 0))
    pick = rows_id == lax.rem(lon + home + lon_count, lon_count)

    def iterate(step, carry):
        rz_old, step_old, ratio_old = carry
        parity = lax.rem(step, 2)
        u_ref = u_pair.at[parity]
        line(lambda k: res_ref[k], lambda k, v: u_ref.__setitem__(k, v), u_ref)
        below, over = interface(u_ref[0], u_ref[top])
        accs = [zero, zero, zero, zero]

        def finish(k):
            value = u_ref[k] + below * resp0[k] + over * resp1[k]
            u_ref[k] = value
            accs[k % 2] = accs[k % 2] + res_ref[k] * value
            return (value, east(value), west(value))

        last = finish(top)
        first = finish(0)
        prev = tuple(from_below(x) for x in last)
        now = first
        for k in range(depth):
            if k < top - 1:
                nxt = finish(k + 1)
            elif k == top - 1:
                nxt = last
            else:
                nxt = tuple(from_above(x) for x in first)
            value = (
                (diag[k] * now[0] - w_e[k] * now[1] - w_w[k] * now[2])
                - (w_n[k] * nxt[0] + w_ne[k] * nxt[1] + w_nw[k] * nxt[2])
                - (w_s[k] * prev[0] + w_se[k] * prev[1] + w_sw[k] * prev[2])
            )
            img[k] = value
            accs[2 + k % 2] = accs[2 + k % 2] + now[0] * value
            prev, now = now, nxt
        rz_part = jnp.sum(jnp.where(own_row, accs[0] + accs[1], 0.0), keepdims=True)
        curve_part = jnp.sum(jnp.where(own_row, accs[2] + accs[3], 0.0), keepdims=True)
        row = jnp.where(own_row, last[0][SUB - 1 :], 0.0)
        row = jnp.where(relative == own, rz_part, row)
        row = jnp.where(relative == own + 1, curve_part, row)
        send_all(parity, row)
        advance(1 - parity, ratio_old, jnp.where(step == 0, 0.0, step_old))
        top_row, rest = wait_all(parity)
        rest_lane = lax.rem(lanes, own)
        fold_image = fold_ref[0] * top_row - fold_ref[1] * facing(top_row)
        rz = jnp.sum(jnp.where(rest_lane == 0, rest, 0.0), keepdims=True)
        curve = jnp.sum(
            jnp.where(rest_lane == 1, rest, 0.0) + fold_image * top_row, keepdims=True
        )
        fix = jnp.sum(jnp.where(pick, fold_image, 0.0), axis=0, keepdims=True)
        img[top] = img[top] + jnp.where(is_top, fix, 0.0)
        ratio = jnp.where(step == 0, 0.0, rz / rz_old)
        length = rz / (curve - ratio * rz / step_old)
        ratio_v = jnp.broadcast_to(ratio, (SUB, width))
        length_v = jnp.broadcast_to(length, (SUB, width))
        for k in range(depth):
            moved = img[k] + ratio_v * along[k]
            along[k] = moved
            res_ref[k] = res_ref[k] - length_v * moved
        return (rz, length, ratio)

    def advance(side, ratio, length):
        ratio_v = jnp.broadcast_to(ratio, (SUB, width))
        length_v = jnp.broadcast_to(length, (SUB, width))
        for k in range(depth):
            toward = u_pair[side, k] + ratio_v * dirn[k]
            dirn[k] = toward
            sol_ref[k] = sol_ref[k] + length_v * toward

    one = jnp.ones((1, 1), jnp.float32)
    u_pair[1] = jnp.zeros((depth, SUB, width), jnp.float32)
    _, length, ratio = lax.fori_loop(0, ITERS, iterate, (one, one, jnp.zeros((1, 1), jnp.float32)))
    advance((ITERS - 1) % 2, ratio, length)

    quarter = depth // 2
    place8 = lax.rem(wide - lat * own + width, width)
    for k in range(quarter):
        row = jnp.where(place8 < own, sol_ref[k], pltpu.roll(res_ref[k], own, 1))
        later = jnp.where(
            place8 < 3 * own,
            pltpu.roll(sol_ref[k + quarter], 2 * own, 1),
            pltpu.roll(res_ref[k + quarter], 3 * own, 1),
        )
        back_msg[pl.ds(k, SUB, stride=quarter), :] = jnp.where(place8 < 2 * own, row, later)
    part = rows // 2

    def back_copy(place):
        return pltpu.make_async_remote_copy(
            src_ref=back_msg.at[place * part : (place + 1) * part],
            dst_ref=back_recv.at[lat],
            send_sem=back_send.at[place],
            recv_sem=back_arrive.at[lat],
            device_id=(place, lon),
            device_id_type=mesh_id,
        )

    for place in range(lat_count):

        @pl.when(lat != place)
        def _(place=place):
            back_copy(place).start()

    back_recv[lat] = back_msg[pl.ds(pl.multiple_of(lat * part, part), part), :]
    for place in range(lat_count):

        @pl.when(lat != place)
        def _(place=place):
            back_copy(place).wait_send()
            pltpu.make_async_remote_copy(
                src_ref=back_msg.at[place * part : (place + 1) * part],
                dst_ref=back_recv.at[place],
                send_sem=back_send.at[place],
                recv_sem=back_arrive.at[place],
                device_id=(place, lon),
                device_id_type=mesh_id,
            ).wait_recv()

    for v in range(part // SUB):
        block, k = divmod(v * SUB, quarter)
        parts = [jnp.zeros((SUB, width), jnp.float32)] * 4
        for place in range(lat_count):
            piece = back_recv[place, v * SUB : (v + 1) * SUB]
            mine = (wide >= place * own) & (wide < (place + 1) * own)
            for i in range(4):
                moved = pltpu.roll(piece, (width - i * own) % width, 1) if i else piece
                parts[i] = jnp.where(mine, moved, parts[i])
        low = block * depth + k
        sol_out[low : low + SUB] = parts[0]
        res_out[low : low + SUB] = parts[1]
        sol_out[low + quarter : low + quarter + SUB] = parts[2]
        res_out[low + quarter : low + quarter + SUB] = parts[3]


def shards(
    right_side,
    surface_term,
    east_coupling,
    north_coupling,
    neast_coupling,
    nwest_coupling,
    land_sea,
    fold_map,
):
    rows, width = right_side.shape
    lat_count = lax.axis_size("lat")
    lon_count = lax.axis_size("lon")
    lon = lax.axis_index("lon")
    n_dev = lat_count * lon_count
    depth = rows * lat_count // SUB
    columns = lon_count * width
    turn = lax.rem(fold_map[:1] + lon * width, columns)

    block = pltpu.VMEM((depth, SUB, width), jnp.float32)
    answer = jax.ShapeDtypeStruct((rows, width), jnp.float32)
    vmem = pl.BlockSpec(memory_space=pltpu.VMEM)
    dma = pltpu.SemaphoreType.DMA

    def held(*shape):
        return pltpu.VMEM((*shape, width), jnp.float32)

    return pl.pallas_call(
        functools.partial(kernel, lat_count, lon_count),
        out_shape=(answer, answer),
        in_specs=[pl.BlockSpec(memory_space=pltpu.SMEM)] + [vmem] * 7,
        out_specs=(vmem, vmem),
        scratch_shapes=[block] * 13
        + [held(2, depth, SUB)]
        + [block] * 5
        + [
            held(7, depth, SUB),
            held(2, 1),
            held(2, n_dev, 1),
            held(2, lon_count),
            held(2),
            held(lon_count, 2),
            held(2, rows),
            held(2, rows),
            held(lat_count, 3, rows),
            held(3, lat_count * rows),
            held(lat_count * rows // 2),
            held(lat_count, rows // 2),
            dma((2,)),
            dma((2,)),
            dma((n_dev,)),
            dma((lon_count,)),
            dma((2,)),
            dma((2,)),
            dma((lat_count,)),
            dma((lat_count,)),
            dma((lat_count,)),
            dma((lat_count,)),
        ],
        compiler_params=pltpu.CompilerParams(collective_id=0, has_side_effects=True),
    )(
        turn,
        right_side,
        surface_term,
        east_coupling,
        north_coupling,
        neast_coupling,
        nwest_coupling,
        land_sea,
    )


def solution(mesh):
    return jax.shard_map(
        shards,
        mesh=mesh,
        in_specs=(P("lat", "lon"),) * 7 + (P("lon"),),
        out_specs=(P("lat", "lon"), P("lat", "lon")),
        check_vma=False,
    )
```
